256 devices in a mesh: row: 8 (over y, z_lo), col: 4 (over x), band: 8 (over z_hi, core).
Axes of the slice: x: 4, y: 4, z: 8 (z_hi: 4, z_lo: 2; z = z_hi * 2 + z_lo), core: 2. Of those that a mesh axis runs over, the one named last changes fastest.
Arguments:
- noisy: float32 [224, 128, 4096], P('band', 'row', 'col'), may hold values from -4 to 4
- weight_map: float32 [128, 4096], P('row', 'col'), may hold values from 1.5 to 12
Outputs:
- denoised: float32 [224, 128, 4096], P('band', 'row', 'col')
The draws below stay inside these ranges and needn't reach their ends.
All inputs are finite; a program needn't handle non-finite values.
Results may differ from the reference program's by a relative error of at most 0.0001.
Values sent between devices are 32-bit elements; how exact they have to be, the bound alone decides.
A program may use at most 64 MiB of HBM per device.

```python
import math
import jax
import jax.numpy as jnp
from jax import lax

BANDS = 224
COLS = 4096
ITERS = 4
ROWS = 128


def draw_noisy(key, part):
    key_center, key_texture = jax.random.split(jax.random.fold_in(key, 17))
    center = jax.random.randint(key_center, (), 0, BANDS).astype(jnp.float32)
    spread = BANDS / 16.0
    texture = jnp.clip(jax.random.normal(key_texture, (BANDS, ROWS, COLS), jnp.float32), -4.0, 4.0)
    offset = (jnp.arange(BANDS, dtype=jnp.float32) - center) / spread
    profile = 0.1 + 0.9 * jnp.exp(-0.5 * offset * offset)
    return (profile[:, None, None] * texture).astype(jnp.float32)


def shard_levels(key, extent, cuts, low, top_value):
    level = 1.0
    for dim, shards_of in cuts:
        steps = jax.random.uniform(jax.random.fold_in(jax.random.fold_in(key, 6), dim), (shards_of,), jnp.float32, low / len(cuts), top_value / len(cuts))
        level = level * jnp.repeat(jnp.exp(steps), extent[dim] // shards_of).reshape((-1,) + (1,) * (len(extent) - 1 - dim))
    return level


def setup_inputs(seed: int = 0) -> dict:
    key_of = jax.random.split(jax.random.key(seed), 3)
    noisy = draw_noisy(jax.random.fold_in(key_of[2], 71), 0)
    weight_map = jnp.clip(jnp.exp(math.log(12.0) - 2.0794415 * jax.random.uniform(key_of[1], (ROWS, COLS), jnp.float32) ** shard_levels(key_of[1], (ROWS, COLS), ((0, 8), (1, 4)), -0.2, 0.2)), 1.5, 12.0)
    return {"noisy": noisy, "weight_map": weight_map}


dual_step = 0.35
primal_step = 0.35

def forward_diff(field):
    zeros_row = jnp.zeros_like(field[:, :1, :])
    zeros_col = jnp.zeros_like(field[:, :, :1])
    grad_x = jnp.concatenate([field[:, 1:, :] - field[:, :-1, :], zeros_row], axis=1)
    grad_y = jnp.concatenate([field[:, :, 1:] - field[:, :, :-1], zeros_col], axis=2)
    return (grad_x, grad_y)

def divergence(first, second):
    masked_a = first.at[:, -1, :].set(0.0)
    masked_b = second.at[:, :, -1].set(0.0)
    above = jnp.concatenate([jnp.zeros_like(masked_a[:, :1, :]), masked_a[:, :-1, :]], axis=1)
    left = jnp.concatenate([jnp.zeros_like(masked_b[:, :, :1]), masked_b[:, :, :-1]], axis=2)
    return masked_a - above + (masked_b - left)

def reference(noisy, weight_map):
    groups = math.gcd(BANDS, 8)
    rows = noisy.shape[1]
    cols = noisy.shape[2]
    source = noisy.reshape(groups, BANDS // groups, rows, cols)
    primal = source
    extra = source
    dual_x = jnp.zeros_like(source)
    dual_y = jnp.zeros_like(source)
    for step in range(ITERS):

        def dual_part(items):
            ubar, first, second = items
            grad_x, grad_y = forward_diff(ubar)
            qx = first + dual_step * grad_x
            qy = second + dual_step * grad_y
            return (qx, qy, lax.optimization_barrier(jnp.sum(qx * qx + qy * qy, axis=0)))
        qxs, qys, partial_value = lax.map(dual_part, (extra, dual_x, dual_y))
        squares = lax.optimization_barrier(jnp.sum(partial_value, axis=0))
        scale = weight_map / jnp.maximum(weight_map, jnp.sqrt(1.0 + squares))

        def primal_part(items):
            qx, qy, older, given = items
            first = scale * qx
            second = scale * qy
            newer = (older + primal_step * divergence(first, second) + primal_step * given) / (1.0 + primal_step)
            return (first, second, newer, 2.0 * newer - older)
        dual_x, dual_y, primal, extra = lax.map(primal_part, (qxs, qys, primal, source))
    return primal.reshape(BANDS, rows, cols)
```

```python
import functools

import jax
import jax.numpy as jnp
from jax import lax
from jax.experimental import pallas as pl
from jax.experimental.pallas import tpu as pltpu
from jax.sharding import PartitionSpec as P

MESH = pl.DeviceIdType.MESH
ITERS = 4
SIGMA = 0.35
TAU = 0.35
C0 = 1.0 / (1.0 + TAU)
KAPPA = TAU / (1.0 + TAU)
M = 4
LANES = 128
RPAD = 8
SROWS = 32
F32 = jnp.float32


def kernel(dims, noisy_ref, weight_ref, out_ref, N, U, UB, PX, PY, QX, QY, SC, MX, MY, OUT,
           PL, PR, RL, RR, SB, RB1, TB, RB2,
           s_in, s_w, sw_s, sw_r, rh_s, rh_r, st_s, st_r, co_s, co_r, ar_s, ar_r, o_l, o_s, o_r):
    nrow, ncol, nband = dims
    bands, rows, cols = noisy_ref.shape
    NB = 2 * bands
    half = cols // 2
    CT = half // LANES
    row = lax.axis_index("row")
    col = lax.axis_index("col")
    band = lax.axis_index("band")
    zc = nband // 2
    z = band // 2
    core = band % 2
    g = col * 2 + core
    ng = ncol * 2

    def dev(r=None, gc=None, zz=None):
        rr = row if r is None else (row + r + nrow) % nrow
        gg = g if gc is None else (g + gc + ng) % ng
        zz = z if zz is None else zz
        return {"row": rr, "col": gg // 2, "band": zz * 2 + gg % 2}

    partner = {"row": row, "col": col, "band": z * 2 + 1 - core}
    up, down, left, right = dev(r=-1), dev(r=1), dev(gc=-1), dev(gc=1)
    corners = (dev(-1, -1), dev(-1, 1), dev(1, -1), dev(1, 1))
    zA = dev(zz=z + 1 - 2 * (z % 2))
    zB = dev(zz=zc - 1 - z)

    loads = []
    for c in range(CT):
        src = noisy_ref.at[:, :, pl.ds(pl.multiple_of(core * half + c * LANES, LANES), LANES)]
        dst = N.at[c, pl.ds(core * bands, bands), RPAD : RPAD + rows, :]
        loads.append(pltpu.make_async_copy(src, dst, s_in.at[c]))
        wsrc = weight_ref.at[:, pl.ds(pl.multiple_of(core * half + c * LANES, LANES), LANES)]
        loads.append(pltpu.make_async_copy(wsrc, N.at[c, NB, RPAD : RPAD + rows, :], s_w.at[c]))
    for cp in loads:
        cp.start()

    barrier = pltpu.get_barrier_semaphore()
    peers = (partner, up, down, left, right, zA, zB) + corners
    for d in peers:
        pl.semaphore_signal(barrier, inc=1, device_id=d, device_id_type=MESH)
    pl.semaphore_wait(barrier, len(peers))

    def remote(src, dst, ss, rs, d):
        return pltpu.make_async_remote_copy(
            src_ref=src, dst_ref=dst, send_sem=ss, recv_sem=rs, device_id=d, device_id_type=MESH
        )

    swaps = []
    for c in range(CT):
        src = noisy_ref.at[:, :, pl.ds(pl.multiple_of((1 - core) * half + c * LANES, LANES), LANES)]
        dst = N.at[c, pl.ds(core * bands, bands), RPAD : RPAD + rows, :]
        swaps.append(remote(src, dst, sw_s.at[c], sw_r.at[c], partner))
    for cp in swaps:
        cp.start()

    lane = lax.broadcasted_iota(jnp.int32, (8, LANES), 1)
    sub = lax.broadcasted_iota(jnp.int32, (8, LANES), 0)
    coef = KAPPA * SIGMA
    for k in range(3):
        for c in range(CT + 1):
            grow = row * rows + (k * 8 - M) + sub
            if c < CT:
                gcol = g * half + c * LANES + lane
            else:
                gcol = g * half + jnp.where(lane < LANES // 2, half + lane, lane - LANES)
            rin = (grow >= 0) & (grow < nrow * rows)
            cin = (gcol >= 0) & (gcol < ng * half)
            kx = (grow >= 0) & (grow < nrow * rows - 1) & cin
            ky = (gcol >= 0) & (gcol < ng * half - 1) & rin
            MX[k, c] = jnp.where(kx, coef, 0.0).astype(F32)
            MY[k, c] = jnp.where(ky, coef, 0.0).astype(F32)

    for cp in loads:
        cp.wait()
    for cp in swaps:
        cp.wait_recv()

    rowh = (
        remote(N.at[0:CT, :, RPAD : RPAD + M, :], N.at[0:CT, :, RPAD + rows : RPAD + rows + M, :], rh_s.at[0], rh_r.at[0], up),
        remote(N.at[0:CT, :, RPAD + rows - M : RPAD + rows, :], N.at[0:CT, :, RPAD - M : RPAD, :], rh_s.at[1], rh_r.at[1], down),
    )
    for cp in rowh:
        cp.start()

    G = 128 // M
    for gi in range(2):
        cnt = min(G, NB + 1 - gi * G)

        def pack(e, acc):
            here = (lane >= e * M) & (lane < e * M + M)
            out = []
            for h in range(2):
                a = N[0, gi * G + e, RPAD + 8 * h : RPAD + 8 * h + 8, :]
                b = N[CT - 1, gi * G + e, RPAD + 8 * h : RPAD + 8 * h + 8, :]
                out.append(jnp.where(here, pltpu.roll(a, e * M, 1), acc[2 * h]))
                out.append(jnp.where(here, pltpu.roll(b, e * M + M, 1), acc[2 * h + 1]))
            return tuple(out)

        zero = jnp.zeros((8, LANES), F32)
        acc = lax.fori_loop(0, cnt, pack, (zero,) * 4)
        for h in range(2):
            PL[gi, 8 * h : 8 * h + 8, :] = acc[2 * h]
            PR[gi, 8 * h : 8 * h + 8, :] = acc[2 * h + 1]

    lo, hi = slice(RPAD, RPAD + rows), RPAD + rows
    strips = [
        remote(PL, RR.at[:, lo, :], st_s.at[0], st_r.at[0], left),
        remote(PR, RL.at[:, lo, :], st_s.at[1], st_r.at[1], right),
        remote(PL.at[:, 0:M, :], RR.at[:, hi : hi + M, :], co_s.at[0], co_r.at[0], corners[0]),
        remote(PR.at[:, 0:M, :], RL.at[:, hi : hi + M, :], co_s.at[1], co_r.at[1], corners[1]),
        remote(PL.at[:, rows - M : rows, :], RR.at[:, RPAD - M : RPAD, :], co_s.at[2], co_r.at[2], corners[2]),
        remote(PR.at[:, rows - M : rows, :], RL.at[:, RPAD - M : RPAD, :], co_s.at[3], co_r.at[3], corners[3]),
    ]
    for cp in strips:
        cp.start()
    for cp in strips:
        cp.wait_recv()
    for gi in range(2):
        cnt = min(G, NB + 1 - gi * G)

        def unpack(e, carry):
            for k in range(3):
                r = RR[gi, RPAD - M + 8 * k : RPAD - M + 8 * k + 8, :]
                l = RL[gi, RPAD - M + 8 * k : RPAD - M + 8 * k + 8, :]
                v = jnp.where(
                    lane < LANES // 2,
                    pltpu.roll(r, (LANES - e * M) % LANES, 1),
                    pltpu.roll(l, LANES - M - e * M, 1),
                )
                N[CT, gi * G + e, RPAD - M + 8 * k : RPAD - M + 8 * k + 8, :] = v
            return carry

        lax.fori_loop(0, cnt, unpack, 0)
    for cp in rowh:
        cp.wait_recv()

    first = lane == 0
    last = lane == LANES - 1
    C = CT + 1

    def rowslice(k, off=0):
        return slice(RPAD - M + 8 * k + off, RPAD - M + 8 * k + 8 + off)

    def dual(it, k):
        src = N if it == 0 else UB
        mx = [MX[k, c] for c in range(C)]
        my = [MY[k, c] for c in range(C)]

        def body(b, acc):
            ub = [src[c, b, rowslice(k), :] for c in range(C)]
            rolled = [pltpu.roll(v, LANES - 1, 1) for v in ub]
            out = []
            for c in range(C):
                below = src[c, b, rowslice(k, 1), :]
                rightv = jnp.where(last, rolled[(c + 1) % C], rolled[c])
                qx = mx[c] * (below - ub[c])
                qy = my[c] * (rightv - ub[c])
                if it > 0:
                    qx = qx + PX[c, b, rowslice(k), :]
                    qy = qy + PY[c, b, rowslice(k), :]
                QX[c, b, rowslice(k), :] = qx
                QY[c, b, rowslice(k), :] = qy
                out.append(acc[c] + (qx * qx + qy * qy))
            return tuple(out)

        acc = lax.fori_loop(0, NB, body, (jnp.zeros((8, LANES), F32),) * C, unroll=2)
        for c in range(C):
            SB[it, k * C + c] = acc[c]

    def primal(it, k):
        sc = [SC[c, rowslice(k), :] for c in range(C)]
        scu = [SC[c, rowslice(k, -1), :] for c in range(C)]

        def body(b, carry):
            py = [sc[c] * QY[c, b, rowslice(k), :] for c in range(C)]
            rolled = [pltpu.roll(v, 1, 1) for v in py]
            for c in range(C):
                px = sc[c] * QX[c, b, rowslice(k), :]
                pxu = scu[c] * QX[c, b, rowslice(k, -1), :]
                pyl = jnp.where(first, rolled[(c - 1) % C], rolled[c])
                div = (px - pxu) + (py[c] - pyl)
                n = N[c, b, rowslice(k), :]
                if it == 0:
                    old = n
                    new = n + div
                else:
                    old = U[c, b, rowslice(k), :]
                    new = C0 * old + (KAPPA * n + div)
                PX[c, b, rowslice(k), :] = px
                PY[c, b, rowslice(k), :] = py[c]
                U[c, b, rowslice(k), :] = new
                UB[c, b, rowslice(k), :] = 2.0 * new - old
            return carry

        lax.fori_loop(0, NB, body, 0, unroll=2)

    def final(k):
        here = slice(RPAD + 8 * k, RPAD + 8 * k + 8)
        above = slice(RPAD + 8 * k - 1, RPAD + 8 * k + 7)
        sc = [SC[c, here, :] for c in range(C)]
        scu = [SC[c, above, :] for c in range(C)]

        def body(b, carry):
            py = [sc[c] * QY[c, b, here, :] for c in range(C)]
            rolled = [pltpu.roll(v, 1, 1) for v in py]
            for c in range(CT):
                px = sc[c] * QX[c, b, here, :]
                pxu = scu[c] * QX[c, b, above, :]
                pyl = jnp.where(first, rolled[(c - 1) % C], rolled[c])
                div = (px - pxu) + (py[c] - pyl)
                OUT[c, b, 8 * k : 8 * k + 8, :] = C0 * U[c, b, here, :] + (KAPPA * N[c, b, here, :] + div)
            return carry

        lax.fori_loop(0, NB, body, 0, unroll=2)

    def scales(it, t0, t1):
        for t in range(t0, t1):
            k, c = divmod(t, C)
            w = N[c, NB, rowslice(k), :]
            s = TB[it, t] + RB2[it, t]
            SC[c, rowslice(k), :] = w / jnp.maximum(w, jnp.sqrt(1.0 + s * (1.0 / (KAPPA * KAPPA))))

    T = 3 * C
    H = 8
    parts = ((0, H), (H, T))
    inflight = []
    for it in range(ITERS):
        def step1(h):
            a, b = parts[h]
            return remote(SB.at[it, a:b], RB1.at[it, a:b], ar_s.at[it, 0, h], ar_r.at[it, 0, h], (zA, zB)[h])

        def step2(h):
            a, b = parts[h]
            return remote(TB.at[it, a:b], RB2.at[it, a:b], ar_s.at[it, 1, h], ar_r.at[it, 1, h], (zB, zA)[h])

        first_copies = [step1(0), step1(1)]
        second_copies = [step2(0), step2(1)]
        dual(it, 0)
        dual(it, 1)
        first_copies[0].start()
        dual(it, 2)
        first_copies[1].start()
        for h in range(2):
            first_copies[h].wait_recv()
            a, b = parts[h]
            for t in range(a, b):
                TB[it, t] = SB[it, t] + RB1[it, t]
            second_copies[h].start()
        second_copies[0].wait_recv()
        scales(it, *parts[0])
        second_copies[1].wait_recv()
        scales(it, *parts[1])
        inflight += first_copies + second_copies
        if it < ITERS - 1:
            for k in range(3):
                primal(it, k)
        else:
            for k in range(2):
                final(k)

    outs = []
    for c in range(CT):
        osrc = OUT.at[c, pl.ds(core * bands, bands)]
        lanes = pl.ds(pl.multiple_of(core * half + c * LANES, LANES), LANES)
        outs.append(pltpu.make_async_copy(osrc, out_ref.at[:, :, lanes], o_l.at[c]))
        osrc = OUT.at[c, pl.ds((1 - core) * bands, bands)]
        outs.append(remote(osrc, out_ref.at[:, :, lanes], o_s.at[c], o_r.at[c], partner))
    for cp in outs:
        cp.start()
    for cp in swaps + list(rowh) + strips + inflight:
        cp.wait_send()
    for cp in outs:
        cp.wait()


def solution(mesh):
    dims = tuple(mesh.shape[a] for a in ("row", "col", "band"))

    def local(noisy, weight_map):
        bands, rows, cols = noisy.shape
        NB = 2 * bands
        CT = cols // 2 // LANES
        C = CT + 1
        vm = lambda *s: pltpu.VMEM(s, F32)
        big = lambda n=NB: vm(C, n, SROWS, LANES)
        dma = lambda *s: pltpu.SemaphoreType.DMA(s)
        return pl.pallas_call(
            functools.partial(kernel, dims),
            out_shape=jax.ShapeDtypeStruct(noisy.shape, F32),
            in_specs=[pl.BlockSpec(memory_space=pl.ANY)] * 2,
            out_specs=pl.BlockSpec(memory_space=pl.ANY),
            scratch_shapes=[
                big(NB + 1), big(), big(), big(), big(), big(), big(),
                vm(C, SROWS, LANES), vm(3, C, 8, LANES), vm(3, C, 8, LANES), vm(CT, NB, rows, LANES),
                vm(2, rows, LANES), vm(2, rows, LANES), vm(2, SROWS, LANES), vm(2, SROWS, LANES),
                vm(ITERS, 16, 8, LANES), vm(ITERS, 16, 8, LANES), vm(ITERS, 16, 8, LANES), vm(ITERS, 16, 8, LANES),
                dma(CT), dma(CT), dma(CT), dma(CT), dma(2), dma(2), dma(2), dma(2), dma(4), dma(4),
                dma(ITERS, 2, 2), dma(ITERS, 2, 2), dma(CT), dma(CT), dma(CT),
            ],
            compiler_params=pltpu.CompilerParams(
                collective_id=0, has_side_effects=True, vmem_limit_bytes=60 * 1024 * 1024
            ),
        )(noisy, weight_map)

    return jax.shard_map(
        local, mesh=mesh, in_specs=(P("band", "row", "col"), P("row", "col")),
        out_specs=P("band", "row", "col"), check_vma=False,
    )
```

```python
import functools

import jax
import jax.numpy as jnp
from jax import lax
from jax.experimental import pallas as pl
from jax.experimental.pallas import tpu as pltpu
from jax.sharding import PartitionSpec as P

MESH = pl.DeviceIdType.MESH
ITERS = 4
SIGMA = 0.35
TAU = 0.35
C0 = 1.0 / (1.0 + TAU)
KAPPA = TAU / (1.0 + TAU)
M = 4
LANES = 128
RPAD = 8
SROWS = 40
F32 = jnp.float32


def kernel(dims, noisy_ref, weight_ref, out_ref, N, U, UB, PX, PY, QX, QY, SC, MX, MY, OUT,
           PL, PR, RL, RR, SB, RB1, TB, RB2,
           s_in, s_w, sw_s, sw_r, rh_s, rh_r, st_s, st_r, co_s, co_r, ar_s, ar_r, o_l, o_s, o_r):
    nrow, ncol, nband = dims
    bands, rows, cols = noisy_ref.shape
    NB = 2 * bands
    half = cols // 2
    CT = half // LANES
    row = lax.axis_index("row")
    col = lax.axis_index("col")
    band = lax.axis_index("band")
    zc = nband // 2
    z = band // 2
    core = band % 2
    g = col * 2 + core
    ng = ncol * 2

    def dev(r=None, gc=None, zz=None):
        rr = row if r is None else (row + r + nrow) % nrow
        gg = g if gc is None else (g + gc + ng) % ng
        zz = z if zz is None else zz
        return {"row": rr, "col": gg // 2, "band": zz * 2 + gg % 2}

    partner = {"row": row, "col": col, "band": z * 2 + 1 - core}
    up, down, left, right = dev(r=-1), dev(r=1), dev(gc=-1), dev(gc=1)
    corners = (dev(-1, -1), dev(-1, 1), dev(1, -1), dev(1, 1))
    zA = dev(zz=z + 1 - 2 * (z % 2))
    zB = dev(zz=zc - 1 - z)

    loads = []
    for c in range(CT):
        src = noisy_ref.at[:, :, pl.ds(pl.multiple_of(core * half + c * LANES, LANES), LANES)]
        dst = N.at[c, pl.ds(core * bands, bands), RPAD : RPAD + rows, :]
        loads.append(pltpu.make_async_copy(src, dst, s_in.at[c]))
        wsrc = weight_ref.at[:, pl.ds(pl.multiple_of(core * half + c * LANES, LANES), LANES)]
        loads.append(pltpu.make_async_copy(wsrc, N.at[c, NB, RPAD : RPAD + rows, :], s_w.at[c]))
    for cp in loads:
        cp.start()

    barrier = pltpu.get_barrier_semaphore()
    peers = (partner, up, down, left, right, zA, zB) + corners
    for d in peers:
        pl.semaphore_signal(barrier, inc=1, device_id=d, device_id_type=MESH)
    pl.semaphore_wait(barrier, len(peers))

    def remote(src, dst, ss, rs, d):
        return pltpu.make_async_remote_copy(
            src_ref=src, dst_ref=dst, send_sem=ss, recv_sem=rs, device_id=d, device_id_type=MESH
        )

    swaps = []
    for c in range(CT):
        src = noisy_ref.at[:, :, pl.ds(pl.multiple_of((1 - core) * half + c * LANES, LANES), LANES)]
        dst = N.at[c, pl.ds(core * bands, bands), RPAD : RPAD + rows, :]
        swaps.append(remote(src, dst, sw_s.at[c], sw_r.at[c], partner))
    for cp in swaps:
        cp.start()

    lane = lax.broadcasted_iota(jnp.int32, (8, LANES), 1)
    sub = lax.broadcasted_iota(jnp.int32, (8, LANES), 0)
    coef = KAPPA * SIGMA
    for k in range(3):
        for c in range(CT + 1):
            grow = row * rows + (k * 8 - M) + sub
            if c < CT:
                gcol = g * half + c * LANES + lane
            else:
                gcol = g * half + jnp.where(lane < LANES // 2, half + lane, lane - LANES)
            rin = (grow >= 0) & (grow < nrow * rows)
            cin = (gcol >= 0) & (gcol < ng * half)
            kx = (grow >= 0) & (grow < nrow * rows - 1) & cin
            ky = (gcol >= 0) & (gcol < ng * half - 1) & rin
            MX[k, c] = jnp.where(kx, coef, 0.0).astype(F32)
            MY[k, c] = jnp.where(ky, coef, 0.0).astype(F32)

    for cp in loads:
        cp.wait()
    for cp in swaps:
        cp.wait_recv()

    G = 128 // M
    for gi in range(2):
        cnt = min(G, NB + 1 - gi * G)

        def pack(e, acc):
            here = (lane >= e * M) & (lane < e * M + M)
            out = []
            for h in range(2):
                a = N[0, gi * G + e, RPAD + 8 * h : RPAD + 8 * h + 8, :]
                b = N[CT - 1, gi * G + e, RPAD + 8 * h : RPAD + 8 * h + 8, :]
                out.append(jnp.where(here, pltpu.roll(a, e * M, 1), acc[2 * h]))
                out.append(jnp.where(here, pltpu.roll(b, e * M + M, 1), acc[2 * h + 1]))
            return tuple(out)

        zero = jnp.zeros((8, LANES), F32)
        acc = lax.fori_loop(0, cnt, pack, (zero,) * 4, unroll=cnt)
        for h in range(2):
            PL[gi, 8 * h : 8 * h + 8, :] = acc[2 * h]
            PR[gi, 8 * h : 8 * h + 8, :] = acc[2 * h + 1]

    lo, hi = slice(RPAD, RPAD + rows), RPAD + rows
    strips = [
        remote(PL, RR.at[:, lo, :], st_s.at[0], st_r.at[0], left),
        remote(PR, RL.at[:, lo, :], st_s.at[1], st_r.at[1], right),
        remote(PL.at[:, 0:M, :], RR.at[:, hi : hi + M, :], co_s.at[0], co_r.at[0], corners[0]),
        remote(PR.at[:, 0:M, :], RL.at[:, hi : hi + M, :], co_s.at[1], co_r.at[1], corners[1]),
        remote(PL.at[:, rows - M : rows, :], RR.at[:, RPAD - M : RPAD, :], co_s.at[2], co_r.at[2], corners[2]),
        remote(PR.at[:, rows - M : rows, :], RL.at[:, RPAD - M : RPAD, :], co_s.at[3], co_r.at[3], corners[3]),
    ]
    for cp in strips:
        cp.start()
    rowh = (
        remote(N.at[0:CT, :, RPAD : RPAD + M, :], N.at[0:CT, :, RPAD + rows : RPAD + rows + M, :], rh_s.at[0], rh_r.at[0], up),
        remote(N.at[0:CT, :, RPAD + rows - M : RPAD + rows, :], N.at[0:CT, :, RPAD - M : RPAD, :], rh_s.at[1], rh_r.at[1], down),
    )
    for cp in rowh:
        cp.start()

    for cp in strips:
        cp.wait_recv()
    for gi in range(2):
        cnt = min(G, NB + 1 - gi * G)

        def unpack(e, carry):
            for k in range(3):
                r = RR[gi, RPAD - M + 8 * k : RPAD - M + 8 * k + 8, :]
                l = RL[gi, RPAD - M + 8 * k : RPAD - M + 8 * k + 8, :]
                v = jnp.where(
                    lane < LANES // 2,
                    pltpu.roll(r, (LANES - e * M) % LANES, 1),
                    pltpu.roll(l, LANES - M - e * M, 1),
                )
                N[CT, gi * G + e, RPAD - M + 8 * k : RPAD - M + 8 * k + 8, :] = v
            return carry

        lax.fori_loop(0, cnt, unpack, 0, unroll=cnt)
    for cp in rowh:
        cp.wait_recv()

    first = lane == 0
    last = lane == LANES - 1
    C = CT + 1

    def rowslice(k, off=0):
        return slice(RPAD - M + 8 * k + off, RPAD - M + 8 * k + 8 + off)

    def dual(it, k):
        src = N if it == 0 else UB
        mx = [MX[k, c] for c in range(C)]
        my = [MY[k, c] for c in range(C)]

        def body(b, acc):
            ub = [src[c, b, rowslice(k), :] for c in range(C)]
            rolled = [pltpu.roll(v, LANES - 1, 1) for v in ub]
            out = []
            for c in range(C):
                below = src[c, b, rowslice(k, 1), :]
                rightv = jnp.where(last, rolled[(c + 1) % C], rolled[c])
                qx = mx[c] * (below - ub[c])
                qy = my[c] * (rightv - ub[c])
                if it > 0:
                    qx = qx + PX[c, b, rowslice(k), :]
                    qy = qy + PY[c, b, rowslice(k), :]
                QX[c, b, rowslice(k), :] = qx
                QY[c, b, rowslice(k), :] = qy
                out.append(acc[c] + (qx * qx + qy * qy))
            return tuple(out)

        acc = lax.fori_loop(0, NB, body, (jnp.zeros((8, LANES), F32),) * C, unroll=14)
        for c in range(C):
            SB[it, k * C + c] = acc[c]

    def primal(it, k):
        sc = [SC[c, rowslice(k), :] for c in range(C)]
        scu = [SC[c, rowslice(k, -1), :] for c in range(C)]

        def body(b, carry):
            py = [sc[c] * QY[c, b, rowslice(k), :] for c in range(C)]
            rolled = [pltpu.roll(v, 1, 1) for v in py]
            for c in range(C):
                px = sc[c] * QX[c, b, rowslice(k), :]
                pxu = scu[c] * QX[c, b, rowslice(k, -1), :]
                pyl = jnp.where(first, rolled[(c - 1) % C], rolled[c])
                div = (px - pxu) + (py[c] - pyl)
                n = N[c, b, rowslice(k), :]
                if it == 0:
                    old = n
                    new = n + div
                else:
                    old = U[c, b, rowslice(k), :]
                    new = C0 * old + (KAPPA * n + div)
                PX[c, b, rowslice(k), :] = px
                PY[c, b, rowslice(k), :] = py[c]
                U[c, b, rowslice(k), :] = new
                UB[c, b, rowslice(k), :] = 2.0 * new - old
            return carry

        lax.fori_loop(0, NB, body, 0, unroll=14)

    def final(k):
        here = slice(RPAD + 8 * k, RPAD + 8 * k + 8)
        above = slice(RPAD + 8 * k - 1, RPAD + 8 * k + 7)
        sc = [SC[c, here, :] for c in range(C)]
        scu = [SC[c, above, :] for c in range(C)]

        def body(b, carry):
            py = [sc[c] * QY[c, b, here, :] for c in range(C)]
            rolled = [pltpu.roll(v, 1, 1) for v in py]
            for c in range(CT):
                px = sc[c] * QX[c, b, here, :]
                pxu = scu[c] * QX[c, b, above, :]
                pyl = jnp.where(first, rolled[(c - 1) % C], rolled[c])
                div = (px - pxu) + (py[c] - pyl)
                OUT[c, b, 8 * k : 8 * k + 8, :] = C0 * U[c, b, here, :] + (KAPPA * N[c, b, here, :] + div)
            return carry

        lax.fori_loop(0, NB, body, 0, unroll=14)

    def scales(it, t0, t1):
        for t in range(t0, t1):
            k, c = divmod(t, C)
            w = N[c, NB, rowslice(k), :]
            s = TB[it, t] + RB2[it, t]
            SC[c, rowslice(k), :] = w / jnp.maximum(w, jnp.sqrt(1.0 + s * (1.0 / (KAPPA * KAPPA))))

    T = 3 * C
    H = 8
    parts = ((0, H), (H, T))
    inflight = []
    for it in range(ITERS):
        def step1(h):
            a, b = parts[h]
            return remote(SB.at[it, a:b], RB1.at[it, a:b], ar_s.at[it, 0, h], ar_r.at[it, 0, h], (zA, zB)[h])

        def step2(h):
            a, b = parts[h]
            return remote(TB.at[it, a:b], RB2.at[it, a:b], ar_s.at[it, 1, h], ar_r.at[it, 1, h], (zB, zA)[h])

        first_copies = [step1(0), step1(1)]
        second_copies = [step2(0), step2(1)]
        dual(it, 0)
        dual(it, 1)
        first_copies[0].start()
        dual(it, 2)
        first_copies[1].start()
        for h in range(2):
            first_copies[h].wait_recv()
            a, b = parts[h]
            for t in range(a, b):
                TB[it, t] = SB[it, t] + RB1[it, t]
            second_copies[h].start()
        second_copies[0].wait_recv()
        scales(it, *parts[0])
        second_copies[1].wait_recv()
        scales(it, *parts[1])
        inflight += first_copies + second_copies
        if it < ITERS - 1:
            for k in range(3):
                primal(it, k)
        else:
            for k in range(2):
                final(k)

    outs = []
    for c in range(CT):
        osrc = OUT.at[c, pl.ds(core * bands, bands)]
        lanes = pl.ds(pl.multiple_of(core * half + c * LANES, LANES), LANES)
        outs.append(pltpu.make_async_copy(osrc, out_ref.at[:, :, lanes], o_l.at[c]))
        osrc = OUT.at[c, pl.ds((1 - core) * bands, bands)]
        outs.append(remote(osrc, out_ref.at[:, :, lanes], o_s.at[c], o_r.at[c], partner))
    for cp in outs:
        cp.start()
    for cp in swaps + list(rowh) + strips + inflight:
        cp.wait_send()
    for cp in outs:
        cp.wait()


def solution(mesh):
    dims = tuple(mesh.shape[a] for a in ("row", "col", "band"))

    def local(noisy, weight_map):
        bands, rows, cols = noisy.shape
        NB = 2 * bands
        CT = cols // 2 // LANES
        C = CT + 1
        vm = lambda *s: pltpu.VMEM(s, F32)
        big = lambda: vm(C, NB + 1, SROWS, LANES)
        dma = lambda *s: pltpu.SemaphoreType.DMA(s)
        return pl.pallas_call(
            functools.partial(kernel, dims),
            out_shape=jax.ShapeDtypeStruct(noisy.shape, F32),
            in_specs=[pl.BlockSpec(memory_space=pl.ANY)] * 2,
            out_specs=pl.BlockSpec(memory_space=pl.ANY),
            scratch_shapes=[
                big(), big(), big(), big(), big(), big(), big(),
                vm(C, SROWS, LANES), vm(3, C, 8, LANES), vm(3, C, 8, LANES), vm(CT, NB, rows, LANES),
                vm(2, rows, LANES), vm(2, rows, LANES), vm(2, SROWS, LANES), vm(2, SROWS, LANES),
                vm(ITERS, 16, 8, LANES), vm(ITERS, 16, 8, LANES), vm(ITERS, 16, 8, LANES), vm(ITERS, 16, 8, LANES),
                dma(CT), dma(CT), dma(CT), dma(CT), dma(2), dma(2), dma(2), dma(2), dma(4), dma(4),
                dma(ITERS, 2, 2), dma(ITERS, 2, 2), dma(CT), dma(CT), dma(CT),
            ],
            compiler_params=pltpu.CompilerParams(
                collective_id=0, has_side_effects=True, vmem_limit_bytes=60 * 1024 * 1024
            ),
        )(noisy, weight_map)

    return jax.shard_map(
        local, mesh=mesh, in_specs=(P("band", "row", "col"), P("row", "col")),
        out_specs=P("band", "row", "col"), check_vma=False,
    )
```

```python
import functools

import jax
import jax.numpy as jnp
from jax import lax
from jax.experimental import pallas as pl
from jax.experimental.pallas import tpu as pltpu
from jax.sharding import PartitionSpec as P

MESH = pl.DeviceIdType.MESH
ITERS = 4
SIGMA = 0.35
TAU = 0.35
C0 = 1.0 / (1.0 + TAU)
KAPPA = TAU / (1.0 + TAU)
M = 4
LANES = 128
F32 = jnp.float32
O0, O1, T2 = 8, 16, 24
SROWS = 40
UNROLL_B = 14
UNROLL_A = 14


def kernel(dims, noisy_ref, weight_ref, out_ref, N, N2, U, UB, PX, PY, QX, QY, SC, ELO, EUP, MX, MY, OUT,
           PL, PR, RL, RR, SB, RB1, TB, RB2,
           s_in, s_w, sw_s, sw_r, g_s, g_r, rh_s, rh_r, st_s, st_r, ar_s, ar_r, e_s, e_r, o_s, o_r):
    nrow, ncol, nband = dims
    bands, rows, cols = noisy_ref.shape
    NB = 2 * bands
    half = cols // 2
    CT = half // LANES
    C = CT + 1
    row = lax.axis_index("row")
    col = lax.axis_index("col")
    band = lax.axis_index("band")
    zc = nband // 2
    z = band // 2
    core = band % 2
    g = col * 2 + core
    ng = ncol * 2

    def dev(r=0, gc=None, zz=None):
        rr = (row + r + nrow) % nrow
        gg = g if gc is None else (gc + ng) % ng
        zz = z if zz is None else zz
        return {"row": rr, "col": gg // 2, "band": zz * 2 + gg % 2}

    partner = {"row": row, "col": col, "band": z * 2 + 1 - core}
    up, down, left, right = dev(-1), dev(1), dev(0, g - 1), dev(0, g + 1)
    corners = (dev(-1, g - 1), dev(-1, g + 1), dev(1, g - 1), dev(1, g + 1))
    iA, iB = z + 1 - 2 * (z % 2), zc - 1 - z
    zA, zB = dev(zz=iA), dev(zz=iB)
    up_zB, down_zA, up_zA, down_zB = dev(-1, zz=iB), dev(1, zz=iA), dev(-1, zz=iA), dev(1, zz=iB)
    mine = pl.ds(core * bands, bands)

    def lanes_of(t, c):
        return pl.ds(pl.multiple_of(t * half + c * LANES, LANES), LANES)

    barrier = pltpu.get_barrier_semaphore()
    peers = (up_zB, down_zA, up_zA, down_zB) + corners + (up, down, zA, zB, left, right)
    for d in peers:
        pl.semaphore_signal(barrier, inc=1, device_id=d, device_id_type=MESH)

    loads = []
    for c in range(CT):
        loads.append(pltpu.make_async_copy(noisy_ref.at[:, :, lanes_of(core, c)], N.at[c, mine, 8 : 8 + rows, :], s_in.at[c]))
        loads.append(pltpu.make_async_copy(weight_ref.at[:, lanes_of(core, c)], N.at[c, NB, 8 : 8 + rows, :], s_w.at[c]))
    for cp in loads:
        cp.start()

    lane = lax.broadcasted_iota(jnp.int32, (8, LANES), 1)
    sub = lax.broadcasted_iota(jnp.int32, (8, LANES), 0)
    coef = KAPPA * SIGMA
    for k in range(3):
        for c in range(C):
            grow = row * rows + (8 * k + sub if k < 2 else jnp.where(sub < M, rows + sub, sub - 8))
            if c < CT:
                gcol = g * half + c * LANES + lane
            else:
                gcol = g * half + jnp.where(lane < LANES // 2, half + lane, lane - LANES)
            rin = (grow >= 0) & (grow < nrow * rows)
            cin = (gcol >= 0) & (gcol < ng * half)
            kx = (grow >= 0) & (grow < nrow * rows - 1) & cin
            ky = (gcol >= 0) & (gcol < ng * half - 1) & rin
            MX[k, c] = jnp.where(kx, coef, 0.0).astype(F32)
            MY[k, c] = jnp.where(ky, coef, 0.0).astype(F32)

    pl.semaphore_wait(barrier, len(peers))

    def remote(src, dst, ss, rs, d):
        return pltpu.make_async_remote_copy(
            src_ref=src, dst_ref=dst, send_sem=ss, recv_sem=rs, device_id=d, device_id_type=MESH
        )

    swaps = []
    for c in range(CT):
        swaps.append(remote(noisy_ref.at[:, :, lanes_of(1 - core, c)], N.at[c, mine, 8 : 8 + rows, :], sw_s.at[c], sw_r.at[c], partner))
    for cp in swaps:
        cp.start()

    def below_piece(t, c):
        return remote(noisy_ref.at[:, 0:1, lanes_of(t, c)], N.at[c, mine, T2 : T2 + 1, :],
                      g_s.at[t, c], g_r.at[core, c], dev(-1, col * 2 + t))

    def below_arrival(t, c):
        at = N.at[c, pl.ds(t * bands, bands), T2 : T2 + 1, :]
        return remote(at, at, g_s.at[t, c], g_r.at[t, c], partner)

    below = [below_piece(t, c) for c in range(CT) for t in range(2)]
    for cp in below:
        cp.start()

    def margin(i, src0, dst, to):
        return remote(N.at[0:CT, 0:NB, 8 + src0[0] : 8 + src0[1], :], dst, rh_s.at[i], rh_r.at[i], to)

    margins = [
        margin(0, (rows - 1, rows), N.at[0:CT, 0:NB, T2 + 7 : T2 + 8, :], down),
        margin(1, (1, 2), N.at[0:CT, 0:NB, T2 + 1 : T2 + 2, :], up),
        margin(2, (rows - 2, rows - 1), N.at[0:CT, 0:NB, T2 + 6 : T2 + 7, :], down),
        margin(3, (2, 4), N2.at[:, :, 2:4, :], up),
        margin(4, (rows - 4, rows - 2), N2.at[:, :, 4:6, :], down),
        remote(N.at[0:CT, NB, 8 : 8 + M, :], N.at[0:CT, NB, T2 : T2 + M, :], rh_s.at[5], rh_r.at[5], up),
        remote(N.at[0:CT, NB, 8 + rows - M : 8 + rows, :], N.at[0:CT, NB, T2 + M : T2 + 2 * M, :], rh_s.at[6], rh_r.at[6], down),
    ]

    for cp in loads:
        cp.wait()
    for cp in swaps:
        cp.wait_recv()

    G = LANES // M
    groups = [(gi, min(G, NB + 1 - gi * G)) for gi in range(2)]
    for gi, cnt in groups:
        acc = [jnp.zeros((8, LANES), F32)] * 4
        for e in range(cnt):
            here = (lane >= e * M) & (lane < e * M + M)
            for h in range(2):
                a = N[0, gi * G + e, 8 + 8 * h : 16 + 8 * h, :]
                b = N[CT - 1, gi * G + e, 8 + 8 * h : 16 + 8 * h, :]
                acc[2 * h] = jnp.where(here, pltpu.roll(a, e * M, 1), acc[2 * h])
                acc[2 * h + 1] = jnp.where(here, pltpu.roll(b, (e * M + M) % LANES, 1), acc[2 * h + 1])
        for h in range(2):
            PL[gi, 8 * h : 8 * h + 8, :] = acc[2 * h]
            PR[gi, 8 * h : 8 * h + 8, :] = acc[2 * h + 1]

    strips = [
        remote(PL, RR.at[:, 0:rows, :], st_s.at[0], st_r.at[0], left),
        remote(PR, RL.at[:, 0:rows, :], st_s.at[1], st_r.at[1], right),
        remote(PL.at[:, 0:M, :], RR.at[:, rows : rows + M, :], st_s.at[2], st_r.at[2], corners[0]),
        remote(PR.at[:, 0:M, :], RL.at[:, rows : rows + M, :], st_s.at[3], st_r.at[3], corners[1]),
        remote(PL.at[:, rows - M : rows, :], RR.at[:, rows + M : rows + 2 * M, :], st_s.at[4], st_r.at[4], corners[2]),
        remote(PR.at[:, rows - M : rows, :], RL.at[:, rows + M : rows + 2 * M, :], st_s.at[5], st_r.at[5], corners[3]),
    ]
    for cp in strips:
        cp.start()
    for cp in (margins[0], margins[5], margins[6]):
        cp.start()

    def unpack(ks):
        for gi, cnt in groups:
            for k in ks:
                r = RR[gi, 8 * k : 8 * k + 8, :]
                l = RL[gi, 8 * k : 8 * k + 8, :]
                for e in range(cnt):
                    N[CT, gi * G + e, 8 + 8 * k : 16 + 8 * k, :] = jnp.where(
                        lane < LANES // 2,
                        pltpu.roll(r, (LANES - e * M) % LANES, 1),
                        pltpu.roll(l, (2 * LANES - M - e * M) % LANES, 1),
                    )

    first = lane == 0
    last = lane == LANES - 1

    def sl(r0, off=0):
        return slice(r0 + off, r0 + off + 8)

    def dual(it, r0):
        k = r0 // 8 - 1
        src = N if it == 0 else UB

        def body(b, acc):
            ub = [src[c, b, sl(r0), :] for c in range(C)]
            rolled = [pltpu.roll(v, LANES - 1, 1) for v in ub]
            out = []
            for c in range(C):
                below = src[c, b, sl(r0, 1), :]
                rightv = jnp.where(last, rolled[(c + 1) % C], rolled[c])
                qx = MX[k, c] * (below - ub[c])
                qy = MY[k, c] * (rightv - ub[c])
                if it > 0:
                    qx = qx + PX[c, b, sl(r0), :]
                    qy = qy + PY[c, b, sl(r0), :]
                QX[c, b, sl(r0), :] = qx
                QY[c, b, sl(r0), :] = qy
                if r0 == T2:
                    QX[c, b, 0:8, :] = qx
                elif it == 0 and r0 == O0:
                    N[c, b, 32:40, :] = ub[c]
                if r0 != T2:
                    out.append(acc[c] + (qx * qx + qy * qy))
            return tuple(out)

        init = () if r0 == T2 else (jnp.zeros((8, LANES), F32),) * C
        acc = lax.fori_loop(0, NB, body, init, unroll=UNROLL_B)
        if r0 != T2:
            for c in range(C):
                SB[it, k * C + c] = acc[c]

    def primal(it, r0):
        sc = [SC[it, c, sl(r0), :] for c in range(C)]
        scu = None if r0 == T2 else [SC[it, c, sl(r0, -1), :] for c in range(C)]

        def body(b, carry):
            py = [sc[c] * QY[c, b, sl(r0), :] for c in range(C)]
            rolled = [pltpu.roll(v, 1, 1) for v in py]
            px = [sc[c] * QX[c, b, sl(r0), :] for c in range(C)]
            for c in range(C):
                PX[c, b, sl(r0), :] = px[c]
            for c in range(C):
                if r0 == T2:
                    pxu = PX[c, b, sl(r0, -1), :]
                else:
                    pxu = scu[c] * QX[c, b, sl(r0, -1), :]
                pyl = jnp.where(first, rolled[(c - 1) % C], rolled[c])
                div = (px[c] - pxu) + (py[c] - pyl)
                n = N[c, b, sl(r0), :]
                if it == 0:
                    old = n
                    new = n + div
                else:
                    old = U[c, b, sl(r0), :]
                    new = C0 * old + (KAPPA * n + div)
                ubar = 2.0 * new - old
                PY[c, b, sl(r0), :] = py[c]
                U[c, b, sl(r0), :] = new
                UB[c, b, sl(r0), :] = ubar
                if r0 == O0:
                    UB[c, b, 32:40, :] = ubar
            return carry

        lax.fori_loop(0, NB, body, 0, unroll=UNROLL_A)

    def final(it, r0, own):
        sc = [SC[it, c, sl(r0), :] for c in range(C)]
        scu = [SC[it, c, sl(r0, -1), :] for c in range(CT)]
        base = (core if own else 1 - core) * bands

        def body(i, carry):
            b = base + i
            py = [sc[c] * QY[c, b, sl(r0), :] for c in range(C)]
            rolled = [pltpu.roll(v, 1, 1) for v in py]
            for c in range(CT):
                px = sc[c] * QX[c, b, sl(r0), :]
                pxu = scu[c] * QX[c, b, sl(r0, -1), :]
                pyl = jnp.where(first, rolled[(c - 1) % C], rolled[c])
                div = (px - pxu) + (py[c] - pyl)
                new = C0 * U[c, b, sl(r0), :] + (KAPPA * N[c, b, sl(r0), :] + div)
                if own:
                    out_ref[i, r0 - 8 : r0, lanes_of(core, c)] = new
                else:
                    OUT[c, i, r0 - 8 : r0, :] = new
            return carry

        lax.fori_loop(0, bands, body, 0, unroll=UNROLL_A)

    pending = list(swaps) + strips + below + margins

    def step(it, n, h):
        src, dst = ((SB, RB1), (TB, RB2))[n]
        a, b = h * C, h * C + C
        return remote(src.at[it, a:b], dst.at[it, a:b], ar_s.at[it, n, h], ar_r.at[it, n, h], (zA, zB)[(n + h) % 2])

    steps = [[[step(it, n, h) for h in range(2)] for n in range(2)] for it in range(ITERS)]

    def edge(it, h, n):
        if h == 0:
            src, dst, to = TB.at[it, 0:C, 0:M, :], ELO.at[it, n, :, 0:M, :], (up, up_zB)[n]
        else:
            src, dst, to = TB.at[it, C : 2 * C, 8 - M : 8, :], EUP.at[it, n, :, 8 - M : 8, :], (down, down_zA)[n]
        return remote(src, dst, e_s.at[it, h, n], e_r.at[it, h, n], to)

    edges = [[[edge(it, h, n) for n in range(2)] for h in range(2)] for it in range(ITERS)]

    def forward(it, h):
        steps[it][0][h].wait_recv()
        for t in range(h * C, h * C + C):
            TB[it, t] = SB[it, t] + RB1[it, t]
        steps[it][1][h].start()
        if h == 1 or it < ITERS - 1:
            for cp in edges[it][h]:
                cp.start()
                pending.append(cp)

    def scale_of(w, s):
        return w / jnp.maximum(w, jnp.sqrt(1.0 + s * (1.0 / (KAPPA * KAPPA))))

    def scales(it, h):
        steps[it][1][h].wait_recv()
        r0 = (O0, O1)[h]
        for c in range(C):
            t = h * C + c
            SC[it, c, sl(r0), :] = scale_of(N[c, NB, sl(r0), :], TB[it, t] + RB2[it, t])

    def scales_above(it):
        for cp in edges[it][1]:
            cp.wait_recv()
        for c in range(C):
            SC[it, c, 0:8, :] = scale_of(N[c, NB, sl(T2), :], EUP[it, 0, c] + EUP[it, 1, c])

    def scales_margin(it):
        for cp in edges[it][0]:
            cp.wait_recv()
        for c in range(C):
            lo = scale_of(N[c, NB, sl(T2), :], ELO[it, 0, c] + ELO[it, 1, c])
            SC[it, c, sl(T2), :] = jnp.where(sub < M, lo, SC[it, c, 0:8, :])

    for cp in strips[:2]:
        cp.wait_recv()
    unpack((0, 1))
    dual(0, O0)
    steps[0][0][0].start()
    for cp in strips[2:]:
        cp.wait_recv()
    unpack((2,))
    for t in range(2):
        for c in range(CT):
            below_arrival(t, c).wait_recv()
    dual(0, O1)
    steps[0][0][1].start()
    margins[1].start()
    margins[2].start()
    for it in range(ITERS):
        pending += steps[it][0] + steps[it][1]
        forward(it, 0)
        forward(it, 1)
        if it == 1:
            for cp in margins[3:5]:
                cp.wait_recv()
            mid = (sub >= 2) & (sub < 6)

            def merge(b, carry):
                for c in range(CT):
                    N[c, b, sl(T2), :] = jnp.where(mid, N2[c, b], N[c, b, sl(T2), :])
                return carry

            lax.fori_loop(0, NB, merge, 0, unroll=8)
            dual(0, T2)
            primal(0, T2)
            dual(1, T2)
        scales(it, 0)
        scales(it, 1)
        if it == ITERS - 1:
            final(it, O1, False)
            scales_above(it)
            final(it, O0, False)
            outs = [
                remote(OUT.at[c], out_ref.at[:, :, lanes_of(core, c)], o_s.at[c], o_r.at[c], partner)
                for c in range(CT)
            ]
            for cp in outs:
                cp.start()
            final(it, O1, True)
            final(it, O0, True)
            continue
        if it == 0:
            margins[3].start()
            margins[4].start()
        primal(it, O1)
        if it == 0:
            for cp in margins[0:3] + margins[5:7]:
                cp.wait_recv()
            dual(0, T2)
        scales_above(it)
        primal(it, O0)
        dual(it + 1, O0)
        steps[it + 1][0][0].start()
        scales_margin(it)
        primal(it, T2)
        dual(it + 1, O1)
        steps[it + 1][0][1].start()
        dual(it + 1, T2)

    for cp in pending:
        cp.wait_send()
    for cp in outs:
        cp.wait()


def solution(mesh):
    dims = tuple(mesh.shape[a] for a in ("row", "col", "band"))

    def local(noisy, weight_map):
        bands, rows, cols = noisy.shape
        NB = 2 * bands
        CT = cols // 2 // LANES
        C = CT + 1
        vm = lambda *s: pltpu.VMEM(s, F32)
        big = lambda: vm(C, NB + 1, SROWS, LANES)
        dma = lambda *s: pltpu.SemaphoreType.DMA(s)
        half_sums = lambda: vm(ITERS, 2 * C, 8, LANES)
        return pl.pallas_call(
            functools.partial(kernel, dims),
            out_shape=jax.ShapeDtypeStruct(noisy.shape, F32),
            in_specs=[pl.BlockSpec(memory_space=pl.ANY)] * 2,
            out_specs=pl.BlockSpec(memory_space=pltpu.VMEM),
            scratch_shapes=[
                big(), vm(CT, NB, 8, LANES), big(), big(), big(), big(), big(), big(),
                vm(ITERS, C, SROWS, LANES), vm(ITERS, 2, C, 8, LANES), vm(ITERS, 2, C, 8, LANES),
                vm(3, C, 8, LANES), vm(3, C, 8, LANES), vm(CT, bands, rows, LANES),
                vm(2, rows, LANES), vm(2, rows, LANES), vm(2, rows + 2 * M, LANES), vm(2, rows + 2 * M, LANES),
                half_sums(), half_sums(), half_sums(), half_sums(),
                dma(CT), dma(CT), dma(CT), dma(CT), dma(2, CT), dma(2, CT), dma(7), dma(7), dma(6), dma(6),
                dma(ITERS, 2, 2), dma(ITERS, 2, 2), dma(ITERS, 2, 2), dma(ITERS, 2, 2), dma(CT), dma(CT),
            ],
            compiler_params=pltpu.CompilerParams(
                collective_id=0, has_side_effects=True, vmem_limit_bytes=52 * 1024 * 1024
            ),
        )(noisy, weight_map)

    return jax.shard_map(
        local, mesh=mesh, in_specs=(P("band", "row", "col"), P("row", "col")),
        out_specs=P("band", "row", "col"), check_vma=False,
    )
```

```python
import functools

import jax
import jax.numpy as jnp
from jax import lax
from jax.experimental import pallas as pl
from jax.experimental.pallas import tpu as pltpu
from jax.sharding import PartitionSpec as P

MESH = pl.DeviceIdType.MESH
ITERS = 4
SIGMA = 0.35
TAU = 0.35
C0 = 1.0 / (1.0 + TAU)
KAPPA = TAU / (1.0 + TAU)
M = 4
LANES = 128
F32 = jnp.float32
O0, O1, T2 = 8, 16, 24
SROWS = 40
UNROLL_B = 14
UNROLL_A = 14


def kernel(dims, noisy_ref, weight_ref, out_ref, N, N2, U, UB, PX, PY, QX, QY, SC, ELO, EUP, MX, MY, OUT,
           E, ST, R, SB, RB1, TB, RB2,
           s_in, s_w, s_e, sw_s, sw_r, g_s, g_r, rh_s, rh_r, st_s, st_r, ar_s, ar_r, e_s, e_r, o_s, o_r):
    nrow, ncol, nband = dims
    bands, rows, cols = noisy_ref.shape
    NB = 2 * bands
    half = cols // 2
    CT = half // LANES
    C = CT + 1
    row = lax.axis_index("row")
    col = lax.axis_index("col")
    band = lax.axis_index("band")
    zc = nband // 2
    z = band // 2
    core = (band + z) % 2
    g = col * 2 + core
    ng = ncol * 2

    def dev(r=0, gc=None, zz=None):
        rr = (row + r + nrow) % nrow
        gg = g if gc is None else (gc + ng) % ng
        zz = z if zz is None else zz
        return {"row": rr, "col": gg // 2, "band": zz * 2 + (gg + zz) % 2}

    partner = {"row": row, "col": col, "band": z * 2 + (1 - core + z) % 2}
    up, down = dev(-1), dev(1)
    iA, iB = z + 1 - 2 * (z % 2), zc - 1 - z
    zA, zB = dev(zz=iA), dev(zz=iB)
    up_zB, down_zA, up_zA, down_zB = dev(-1, zz=iB), dev(1, zz=iA), dev(-1, zz=iA), dev(1, zz=iB)
    mine = pl.ds(core * bands, bands)

    def lanes_of(t, c):
        return pl.ds(pl.multiple_of(t * half + c * LANES, LANES), LANES)

    barrier = pltpu.get_barrier_semaphore()
    beside = [(r, d) for d in (-2, -1, 1, 2) for r in (-1, 1, 0)]
    peers = [up_zB, down_zA, up_zA, down_zB] + [dev(r, g + d) for r, d in beside] + [up, down, zA, zB]
    for d in peers:
        pl.semaphore_signal(barrier, inc=1, device_id=d, device_id_type=MESH)

    loads = []
    for c in range(CT):
        loads.append(pltpu.make_async_copy(noisy_ref.at[:, :, lanes_of(core, c)], N.at[c, mine, 8 : 8 + rows, :], s_in.at[c]))
        loads.append(pltpu.make_async_copy(weight_ref.at[:, lanes_of(core, c)], N.at[c, NB, 8 : 8 + rows, :], s_w.at[c]))
    for i, at in enumerate(((CT - 1) * (1 - core), (CT - 1) * core)):
        lanes = pl.ds(pl.multiple_of((1 - core) * half + at * LANES, LANES), LANES)
        loads.append(pltpu.make_async_copy(noisy_ref.at[:, :, lanes], E.at[i], s_e.at[i]))
    for cp in loads:
        cp.start()

    lane = lax.broadcasted_iota(jnp.int32, (8, LANES), 1)
    sub = lax.broadcasted_iota(jnp.int32, (8, LANES), 0)
    coef = KAPPA * SIGMA
    for k in range(3):
        for c in range(C):
            grow = row * rows + (8 * k + sub if k < 2 else jnp.where(sub < M, rows + sub, sub - 8))
            if c < CT:
                gcol = g * half + c * LANES + lane
            else:
                gcol = g * half + jnp.where(lane < LANES // 2, half + lane, lane - LANES)
            rin = (grow >= 0) & (grow < nrow * rows)
            cin = (gcol >= 0) & (gcol < ng * half)
            kx = (grow >= 0) & (grow < nrow * rows - 1) & cin
            ky = (gcol >= 0) & (gcol < ng * half - 1) & rin
            MX[k, c] = jnp.where(kx, coef, 0.0).astype(F32)
            MY[k, c] = jnp.where(ky, coef, 0.0).astype(F32)

    for cp in loads:
        cp.wait()

    for h in range(2):
        tile_rows = slice(8 + 8 * h, 16 + 8 * h)
        acc = [jnp.zeros((8, LANES), F32)] * 4
        for e in range(bands + 1):
            here = (lane >= e * M) & (lane < e * M + M)
            own = core * bands + e if e < bands else NB
            acc[0] = jnp.where(here, pltpu.roll(N[0, own, tile_rows, :], e * M, 1), acc[0])
            acc[1] = jnp.where(here, pltpu.roll(N[CT - 1, own, tile_rows, :], (e * M + M) % LANES, 1), acc[1])
            if e < bands:
                acc[2] = jnp.where(here, pltpu.roll(E[0, e, 8 * h : 8 * h + 8, :], e * M + M * (1 - core), 1), acc[2])
                acc[3] = jnp.where(here, pltpu.roll(E[1, e, 8 * h : 8 * h + 8, :], e * M + M * core, 1), acc[3])
        for i in range(4):
            ST[i, 8 * h : 8 * h + 8, :] = acc[i]
        R[core, core, 8 * h : 8 * h + 8, :] = acc[3]

    pl.semaphore_wait(barrier, len(peers))

    def remote(src, dst, ss, rs, d):
        return pltpu.make_async_remote_copy(
            src_ref=src, dst_ref=dst, send_sem=ss, recv_sem=rs, device_id=d, device_id_type=MESH
        )

    swaps = []
    for c in range(CT):
        swaps.append(remote(noisy_ref.at[:, :, lanes_of(1 - core, c)], N.at[c, mine, 8 : 8 + rows, :], sw_s.at[c], sw_r.at[c], partner))
    for cp in swaps:
        cp.start()

    strips = []
    for i, (side, shift) in enumerate(((0, -1), (1, 1), (1 - core, 2 - 4 * core), (core, 0))):
        for part, (r, src, dst) in enumerate(((0, 0, 0), (-1, 0, rows), (1, rows - M, rows + M))):
            if i == 3 and part == 0:
                continue
            n = rows if part == 0 else M
            strips.append(remote(ST.at[i, src : src + n, :], R.at[side, core, dst : dst + n, :],
                                 st_s.at[i, part], st_r.at[side, core, part], dev(r, g + shift)))
    for cp in strips:
        cp.start()

    def strip_arrival(side, src, part):
        n = rows if part == 0 else M
        at = R.at[side, src, (0, rows, rows + M)[part] : (0, rows, rows + M)[part] + n, :]
        return remote(at, at, st_s.at[0, 0], st_r.at[side, src, part], partner)

    def next_row(d, t, c):
        src0, dst0 = (0, 0) if d == 0 else (rows - 1, 2 * M - 1)
        return remote(noisy_ref.at[:, src0 : src0 + 1, lanes_of(t, c)], N.at[c, mine, T2 + dst0 : T2 + dst0 + 1, :],
                      g_s.at[d, t, c], g_r.at[d, core, c], dev(-1 if d == 0 else 1, col * 2 + t))

    def next_row_arrival(d, t, c):
        at = N.at[c, pl.ds(t * bands, bands), T2 + (2 * M - 1) * d : T2 + (2 * M - 1) * d + 1, :]
        return remote(at, at, g_s.at[d, t, c], g_r.at[d, t, c], partner)

    nexts = [next_row(d, t, c) for d in range(2) for c in range(CT) for t in range(2)]
    for cp in nexts:
        cp.start()

    def margin(i, src0, dst, dst0, to):
        return remote(N.at[0:CT, 0:NB, 8 + src0 : 9 + src0, :], dst.at[0:CT, 0:NB, dst0 : dst0 + 1, :], rh_s.at[i], rh_r.at[i], to)

    margins = [
        margin(0, 1, N, T2 + 1, up),
        margin(1, rows - 2, N, T2 + 6, down),
        margin(2, 2, N2, 2, up),
        margin(3, rows - 3, N2, 5, down),
        margin(4, 3, N2, 3, up),
        margin(5, rows - 4, N2, 4, down),
        remote(N.at[0:CT, NB, 8 : 8 + M, :], N.at[0:CT, NB, T2 : T2 + M, :], rh_s.at[6], rh_r.at[6], up),
        remote(N.at[0:CT, NB, 8 + rows - M : 8 + rows, :], N.at[0:CT, NB, T2 + M : T2 + 2 * M, :], rh_s.at[7], rh_r.at[7], down),
    ]

    for cp in (margins[6], margins[7]):
        cp.start()
    for cp in swaps:
        cp.wait_recv()
    margins[0].start()

    def unpack(ks):
        for k in ks:
            for src in range(2):
                right = R[0, src, 8 * k : 8 * k + 8, :]
                left = R[1, src, 8 * k : 8 * k + 8, :]
                for e in range(bands):
                    N[CT, src * bands + e, 8 + 8 * k : 16 + 8 * k, :] = jnp.where(
                        lane < LANES // 2,
                        pltpu.roll(right, (LANES - e * M) % LANES, 1),
                        pltpu.roll(left, (2 * LANES - M - e * M) % LANES, 1),
                    )
            N[CT, NB, 8 + 8 * k : 16 + 8 * k, :] = jnp.where(
                lane < LANES // 2,
                pltpu.roll(R[0, 1 - core, 8 * k : 8 * k + 8, :], LANES - bands * M, 1),
                pltpu.roll(R[1, 1 - core, 8 * k : 8 * k + 8, :], LANES - M - bands * M, 1),
            )

    first = lane == 0
    last = lane == LANES - 1

    def sl(r0, off=0):
        return slice(r0 + off, r0 + off + 8)

    def dual(it, r0):
        k = r0 // 8 - 1
        src = N if it == 0 else UB

        def body(b, acc):
            ub = [src[c, b, sl(r0), :] for c in range(C)]
            rolled = [pltpu.roll(v, LANES - 1, 1) for v in ub]
            out = []
            for c in range(C):
                below = src[c, b, sl(r0, 1), :]
                rightv = jnp.where(last, rolled[(c + 1) % C], rolled[c])
                qx = MX[k, c] * (below - ub[c])
                qy = MY[k, c] * (rightv - ub[c])
                if it > 0:
                    qx = qx + PX[c, b, sl(r0), :]
                    qy = qy + PY[c, b, sl(r0), :]
                QX[c, b, sl(r0), :] = qx
                QY[c, b, sl(r0), :] = qy
                if r0 == T2:
                    QX[c, b, 0:8, :] = qx
                elif it == 0 and r0 == O0:
                    N[c, b, 32:40, :] = ub[c]
                if r0 != T2:
                    out.append(acc[c] + (qx * qx + qy * qy))
            return tuple(out)

        init = () if r0 == T2 else (jnp.zeros((8, LANES), F32),) * C
        acc = lax.fori_loop(0, NB, body, init, unroll=UNROLL_B)
        if r0 != T2:
            for c in range(C):
                SB[it, k * C + c] = acc[c]

    def primal(it, r0):
        sc = [SC[it, c, sl(r0), :] for c in range(C)]
        scu = None if r0 == T2 else [SC[it, c, sl(r0, -1), :] for c in range(C)]

        def body(b, carry):
            py = [sc[c] * QY[c, b, sl(r0), :] for c in range(C)]
            rolled = [pltpu.roll(v, 1, 1) for v in py]
            px = [sc[c] * QX[c, b, sl(r0), :] for c in range(C)]
            for c in range(C):
                PX[c, b, sl(r0), :] = px[c]
            for c in range(C):
                if r0 == T2:
                    pxu = PX[c, b, sl(r0, -1), :]
                else:
                    pxu = scu[c] * QX[c, b, sl(r0, -1), :]
                pyl = jnp.where(first, rolled[(c - 1) % C], rolled[c])
                div = (px[c] - pxu) + (py[c] - pyl)
                n = N[c, b, sl(r0), :]
                if it == 0:
                    old = n
                    new = n + div
                else:
                    old = U[c, b, sl(r0), :]
                    new = C0 * old + (KAPPA * n + div)
                ubar = 2.0 * new - old
                PY[c, b, sl(r0), :] = py[c]
                U[c, b, sl(r0), :] = new
                UB[c, b, sl(r0), :] = ubar
                if r0 == O0:
                    UB[c, b, 32:40, :] = ubar
            return carry

        lax.fori_loop(0, NB, body, 0, unroll=UNROLL_A)

    def final(it, r0, own):
        sc = [SC[it, c, sl(r0), :] for c in range(C)]
        scu = [SC[it, c, sl(r0, -1), :] for c in range(CT)]
        base = (core if own else 1 - core) * bands

        def body(i, carry):
            b = base + i
            py = [sc[c] * QY[c, b, sl(r0), :] for c in range(C)]
            rolled = [pltpu.roll(v, 1, 1) for v in py]
            for c in range(CT):
                px = sc[c] * QX[c, b, sl(r0), :]
                pxu = scu[c] * QX[c, b, sl(r0, -1), :]
                pyl = jnp.where(first, rolled[(c - 1) % C], rolled[c])
                div = (px - pxu) + (py[c] - pyl)
                new = C0 * U[c, b, sl(r0), :] + (KAPPA * N[c, b, sl(r0), :] + div)
                if own:
                    out_ref[i, r0 - 8 : r0, lanes_of(core, c)] = new
                else:
                    OUT[c, i, r0 - 8 : r0, :] = new
            return carry

        lax.fori_loop(0, bands, body, 0, unroll=UNROLL_A)

    pending = list(swaps) + strips + nexts + margins

    def step(it, n, h):
        src, dst = ((SB, RB1), (TB, RB2))[n]
        a, b = h * C, h * C + C
        return remote(src.at[it, a:b], dst.at[it, a:b], ar_s.at[it, n, h], ar_r.at[it, n, h], (zA, zB)[(n + h) % 2])

    steps = [[[step(it, n, h) for h in range(2)] for n in range(2)] for it in range(ITERS)]

    def edge(it, h, n):
        if h == 0:
            src, dst, to = TB.at[it, 0:C, 0:M, :], ELO.at[it, n, :, 0:M, :], (up, up_zB)[n]
        else:
            src, dst, to = TB.at[it, C : 2 * C, 8 - M : 8, :], EUP.at[it, n, :, 8 - M : 8, :], (down, down_zA)[n]
        return remote(src, dst, e_s.at[it, h, n], e_r.at[it, h, n], to)

    edges = [[[edge(it, h, n) for n in range(2)] for h in range(2)] for it in range(ITERS)]

    def forward(it, h):
        steps[it][0][h].wait_recv()
        for t in range(h * C, h * C + C):
            TB[it, t] = SB[it, t] + RB1[it, t]
        steps[it][1][h].start()
        if h == 1 or it < ITERS - 1:
            for cp in edges[it][h]:
                cp.start()
                pending.append(cp)

    def scale_of(w, s):
        return w / jnp.maximum(w, jnp.sqrt(1.0 + s * (1.0 / (KAPPA * KAPPA))))

    def scales(it, h):
        steps[it][1][h].wait_recv()
        r0 = (O0, O1)[h]
        for c in range(C):
            t = h * C + c
            SC[it, c, sl(r0), :] = scale_of(N[c, NB, sl(r0), :], TB[it, t] + RB2[it, t])

    def scales_above(it):
        for cp in edges[it][1]:
            cp.wait_recv()
        for c in range(C):
            SC[it, c, 0:8, :] = scale_of(N[c, NB, sl(T2), :], EUP[it, 0, c] + EUP[it, 1, c])

    def scales_margin(it):
        for cp in edges[it][0]:
            cp.wait_recv()
        for c in range(C):
            lo = scale_of(N[c, NB, sl(T2), :], ELO[it, 0, c] + ELO[it, 1, c])
            SC[it, c, sl(T2), :] = jnp.where(sub < M, lo, SC[it, c, 0:8, :])

    for side, src in ((core, 1 - core), (1 - core, 0), (1 - core, 1)):
        strip_arrival(side, src, 0).wait_recv()
    unpack((0, 1))
    dual(0, O0)
    steps[0][0][0].start()
    for side in range(2):
        for src in range(2):
            for part in (1, 2):
                strip_arrival(side, src, part).wait_recv()
    unpack((2,))
    for t in range(2):
        for c in range(CT):
            next_row_arrival(0, t, c).wait_recv()
    dual(0, O1)
    steps[0][0][1].start()
    margins[1].start()
    for it in range(ITERS):
        pending += steps[it][0] + steps[it][1]
        order = (0, 1) if it == 0 else (1, 0)
        for h in order:
            forward(it, h)
        if it == 0:
            for cp in margins[2:5]:
                cp.start()
        if it == 1:
            for cp in margins[2:6]:
                cp.wait_recv()
            mid = (sub >= 2) & (sub < 6)

            def merge(b, carry):
                for c in range(CT):
                    N[c, b, sl(T2), :] = jnp.where(mid, N2[c, b], N[c, b, sl(T2), :])
                return carry

            lax.fori_loop(0, NB, merge, 0, unroll=8)
            dual(0, T2)
            primal(0, T2)
            dual(1, T2)
        for h in order:
            scales(it, h)
        if it == ITERS - 1:
            final(it, O1, False)
            outs = [
                remote(OUT.at[c, :, 8 * h : 8 * h + 8, :], out_ref.at[:, 8 * h : 8 * h + 8, lanes_of(core, c)], o_s.at[h, c], o_r.at[h, c], partner)
                for h in (1, 0) for c in range(CT)
            ]
            for cp in outs[:CT]:
                cp.start()
            scales_above(it)
            final(it, O0, False)
            for cp in outs[CT:]:
                cp.start()
            final(it, O1, True)
            final(it, O0, True)
            continue
        primal(it, O1)
        if it == 0:
            for t in range(2):
                for c in range(CT):
                    next_row_arrival(1, t, c).wait_recv()
            for cp in margins[0:2] + margins[6:8]:
                cp.wait_recv()
            dual(0, T2)
        scales_above(it)
        primal(it, O0)
        scales_margin(it)
        primal(it, T2)
        dual(it + 1, O1)
        steps[it + 1][0][1].start()
        dual(it + 1, O0)
        steps[it + 1][0][0].start()
        if it == 0:
            margins[5].start()
        dual(it + 1, T2)

    for cp in pending:
        cp.wait_send()
    for cp in outs:
        cp.wait()


def solution(mesh):
    dims = tuple(mesh.shape[a] for a in ("row", "col", "band"))

    def local(noisy, weight_map):
        bands, rows, cols = noisy.shape
        NB = 2 * bands
        CT = cols // 2 // LANES
        C = CT + 1
        vm = lambda *s: pltpu.VMEM(s, F32)
        big = lambda: vm(C, NB + 1, SROWS, LANES)
        dma = lambda *s: pltpu.SemaphoreType.DMA(s)
        half_sums = lambda: vm(ITERS, 2 * C, 8, LANES)
        return pl.pallas_call(
            functools.partial(kernel, dims),
            out_shape=jax.ShapeDtypeStruct(noisy.shape, F32),
            in_specs=[pl.BlockSpec(memory_space=pl.ANY)] * 2,
            out_specs=pl.BlockSpec(memory_space=pltpu.VMEM),
            scratch_shapes=[
                big(), vm(CT, NB, 8, LANES), big(), big(), big(), big(), big(), big(),
                vm(ITERS, C, SROWS, LANES), vm(ITERS, 2, C, 8, LANES), vm(ITERS, 2, C, 8, LANES),
                vm(3, C, 8, LANES), vm(3, C, 8, LANES), vm(CT, bands, rows, LANES),
                vm(2, bands, rows, LANES), vm(4, rows, LANES), vm(2, 2, rows + 2 * M, LANES),
                half_sums(), half_sums(), half_sums(), half_sums(),
                dma(CT), dma(CT), dma(2), dma(CT), dma(CT), dma(2, 2, CT), dma(2, 2, CT), dma(8), dma(8), dma(4, 3), dma(2, 2, 3),
                dma(ITERS, 2, 2), dma(ITERS, 2, 2), dma(ITERS, 2, 2), dma(ITERS, 2, 2), dma(2, CT), dma(2, CT),
            ],
            compiler_params=pltpu.CompilerParams(
                collective_id=0, has_side_effects=True, vmem_limit_bytes=52 * 1024 * 1024
            ),
        )(noisy, weight_map)

    return jax.shard_map(
        local, mesh=mesh, in_specs=(P("band", "row", "col"), P("row", "col")),
        out_specs=P("band", "row", "col"), check_vma=False,
    )
```

```python
import functools

import jax
import jax.numpy as jnp
from jax import lax
from jax.experimental import pallas as pl
from jax.experimental.pallas import tpu as pltpu
from jax.sharding import PartitionSpec as P

MESH = pl.DeviceIdType.MESH
ITERS = 4
SIGMA = 0.35
TAU = 0.35
C0 = 1.0 / (1.0 + TAU)
KAPPA = TAU / (1.0 + TAU)
M = 4
LANES = 128
F32 = jnp.float32
O0, O1, T2 = 8, 16, 24
SROWS = 40
UNROLL_B = 28
UNROLL_A = 14


def kernel(dims, noisy_ref, weight_ref, out_ref, N, N2, U, UB, PX, QX, QY, SC, ELO, EUP, MX, MY, OUT,
           E, ST, R, SB, RB1, TB, RB2,
           s_in, s_w, s_e, sw_s, sw_r, g_s, g_r, rh_s, rh_r, st_s, st_r, ar_s, ar_r, e_s, e_r, o_s, o_r):
    nrow, ncol, nband = dims
    bands, rows, cols = noisy_ref.shape
    NB = 2 * bands
    half = cols // 2
    CT = half // LANES
    C = CT + 1
    row = lax.axis_index("row")
    col = lax.axis_index("col")
    band = lax.axis_index("band")
    zc = nband // 2
    z = band // 2
    core = (band + z) % 2
    g = col * 2 + core
    ng = ncol * 2

    def dev(r=0, gc=None, zz=None):
        rr = (row + r + nrow) % nrow
        gg = g if gc is None else (gc + ng) % ng
        zz = z if zz is None else zz
        return {"row": rr, "col": gg // 2, "band": zz * 2 + (gg + zz) % 2}

    partner = {"row": row, "col": col, "band": z * 2 + (1 - core + z) % 2}
    up, down = dev(-1), dev(1)
    iA, iB = z + 1 - 2 * (z % 2), zc - 1 - z
    zA, zB = dev(zz=iA), dev(zz=iB)
    up_zB, down_zA, up_zA, down_zB = dev(-1, zz=iB), dev(1, zz=iA), dev(-1, zz=iA), dev(1, zz=iB)
    mine = pl.ds(core * bands, bands)

    def lanes_of(t, c):
        return pl.ds(pl.multiple_of(t * half + c * LANES, LANES), LANES)

    barrier = pltpu.get_barrier_semaphore()
    beside = [(r, d) for d in (-2, -1, 1, 2) for r in (-1, 1, 0)]
    peers = [up_zB, down_zA, up_zA, down_zB] + [dev(r, g + d) for r, d in beside] + [up, down, zA, zB]
    for d in peers:
        pl.semaphore_signal(barrier, inc=1, device_id=d, device_id_type=MESH)

    loads = []
    for c in range(CT):
        loads.append(pltpu.make_async_copy(noisy_ref.at[:, :, lanes_of(core, c)], N.at[c, mine, 8 : 8 + rows, :], s_in.at[c]))
        loads.append(pltpu.make_async_copy(weight_ref.at[:, lanes_of(core, c)], N.at[c, NB, 8 : 8 + rows, :], s_w.at[c]))
    for i, at in enumerate(((CT - 1) * (1 - core), (CT - 1) * core)):
        lanes = pl.ds(pl.multiple_of((1 - core) * half + at * LANES, LANES), LANES)
        loads.append(pltpu.make_async_copy(noisy_ref.at[:, :, lanes], E.at[i], s_e.at[i]))
    for cp in loads:
        cp.start()

    lane = lax.broadcasted_iota(jnp.int32, (8, LANES), 1)
    sub = lax.broadcasted_iota(jnp.int32, (8, LANES), 0)
    coef = KAPPA * SIGMA
    for k in range(3):
        for c in range(C):
            grow = row * rows + (8 * k + sub if k < 2 else jnp.where(sub < M, rows + sub, sub - 8))
            if c < CT:
                gcol = g * half + c * LANES + lane
            else:
                gcol = g * half + jnp.where(lane < LANES // 2, half + lane, lane - LANES)
            rin = (grow >= 0) & (grow < nrow * rows)
            cin = (gcol >= 0) & (gcol < ng * half)
            kx = (grow >= 0) & (grow < nrow * rows - 1) & cin
            ky = (gcol >= 0) & (gcol < ng * half - 1) & rin
            MX[k, c] = jnp.where(kx, coef, 0.0).astype(F32)
            MY[k, c] = jnp.where(ky, coef, 0.0).astype(F32)

    for cp in loads:
        cp.wait()

    for h in range(2):
        tile_rows = slice(8 + 8 * h, 16 + 8 * h)
        acc = [jnp.zeros((8, LANES), F32)] * 4
        for e in range(bands + 1):
            here = (lane >= e * M) & (lane < e * M + M)
            own = core * bands + e if e < bands else NB
            acc[0] = jnp.where(here, pltpu.roll(N[0, own, tile_rows, :], e * M, 1), acc[0])
            acc[1] = jnp.where(here, pltpu.roll(N[CT - 1, own, tile_rows, :], (e * M + M) % LANES, 1), acc[1])
            if e < bands:
                acc[2] = jnp.where(here, pltpu.roll(E[0, e, 8 * h : 8 * h + 8, :], e * M + M * (1 - core), 1), acc[2])
                acc[3] = jnp.where(here, pltpu.roll(E[1, e, 8 * h : 8 * h + 8, :], e * M + M * core, 1), acc[3])
        for i in range(4):
            ST[i, 8 * h : 8 * h + 8, :] = acc[i]
        R[core, core, 8 * h : 8 * h + 8, :] = acc[3]

    pl.semaphore_wait(barrier, len(peers))

    def remote(src, dst, ss, rs, d):
        return pltpu.make_async_remote_copy(
            src_ref=src, dst_ref=dst, send_sem=ss, recv_sem=rs, device_id=d, device_id_type=MESH
        )

    swaps = []
    for c in range(CT):
        swaps.append(remote(noisy_ref.at[:, :, lanes_of(1 - core, c)], N.at[c, mine, 8 : 8 + rows, :], sw_s.at[c], sw_r.at[c], partner))
    for cp in swaps:
        cp.start()

    strips = []
    for i, (side, shift) in enumerate(((0, -1), (1, 1), (1 - core, 2 - 4 * core), (core, 0))):
        for part, (r, src, dst) in enumerate(((0, 0, 0), (-1, 0, rows), (1, rows - M, rows + M))):
            if i == 3 and part == 0:
                continue
            n = rows if part == 0 else M
            strips.append(remote(ST.at[i, src : src + n, :], R.at[side, core, dst : dst + n, :],
                                 st_s.at[i, part], st_r.at[side, core, part], dev(r, g + shift)))
    for cp in strips:
        cp.start()

    def strip_arrival(side, src, part):
        n = rows if part == 0 else M
        at = R.at[side, src, (0, rows, rows + M)[part] : (0, rows, rows + M)[part] + n, :]
        return remote(at, at, st_s.at[0, 0], st_r.at[side, src, part], partner)

    def next_row(d, t, c):
        src0, dst0 = (0, 0) if d == 0 else (rows - 1, 2 * M - 1)
        return remote(noisy_ref.at[:, src0 : src0 + 1, lanes_of(t, c)], N.at[c, mine, T2 + dst0 : T2 + dst0 + 1, :],
                      g_s.at[d, t, c], g_r.at[d, core, c], dev(-1 if d == 0 else 1, col * 2 + t))

    def next_row_arrival(d, t, c):
        at = N.at[c, pl.ds(t * bands, bands), T2 + (2 * M - 1) * d : T2 + (2 * M - 1) * d + 1, :]
        return remote(at, at, g_s.at[d, t, c], g_r.at[d, t, c], partner)

    nexts = [next_row(d, t, c) for d in range(2) for c in range(CT) for t in range(2)]
    for cp in nexts:
        cp.start()

    def margin(i, src0, dst, dst0, to):
        return remote(N.at[0:CT, 0:NB, 8 + src0 : 9 + src0, :], dst.at[0:CT, 0:NB, dst0 : dst0 + 1, :], rh_s.at[i], rh_r.at[i], to)

    margins = [
        margin(0, 1, N, T2 + 1, up),
        margin(1, rows - 2, N, T2 + 6, down),
        margin(2, 2, N2, 2, up),
        margin(3, rows - 3, N2, 5, down),
        margin(4, 3, N2, 3, up),
        margin(5, rows - 4, N2, 4, down),
        remote(N.at[0:CT, NB, 8 : 8 + M, :], N.at[0:CT, NB, T2 : T2 + M, :], rh_s.at[6], rh_r.at[6], up),
        remote(N.at[0:CT, NB, 8 + rows - M : 8 + rows, :], N.at[0:CT, NB, T2 + M : T2 + 2 * M, :], rh_s.at[7], rh_r.at[7], down),
    ]

    for cp in (margins[6], margins[7]):
        cp.start()
    for cp in swaps:
        cp.wait_recv()
    margins[0].start()

    def unpack(ks):
        for k in ks:
            for src in range(2):
                right = R[0, src, 8 * k : 8 * k + 8, :]
                left = R[1, src, 8 * k : 8 * k + 8, :]
                for e in range(bands):
                    N[CT, src * bands + e, 8 + 8 * k : 16 + 8 * k, :] = jnp.where(
                        lane < LANES // 2,
                        pltpu.roll(right, (LANES - e * M) % LANES, 1),
                        pltpu.roll(left, (2 * LANES - M - e * M) % LANES, 1),
                    )
            N[CT, NB, 8 + 8 * k : 16 + 8 * k, :] = jnp.where(
                lane < LANES // 2,
                pltpu.roll(R[0, 1 - core, 8 * k : 8 * k + 8, :], LANES - bands * M, 1),
                pltpu.roll(R[1, 1 - core, 8 * k : 8 * k + 8, :], LANES - M - bands * M, 1),
            )

    first = lane == 0
    last = lane == LANES - 1

    def sl(r0, off=0):
        return slice(r0 + off, r0 + off + 8)

    def dual(it, r0):
        k = r0 // 8 - 1
        src = N if it == 0 else UB

        def body(b, acc):
            ub = [src[c, b, sl(r0), :] for c in range(C)]
            rolled = [pltpu.roll(v, LANES - 1, 1) for v in ub]
            out = []
            for c in range(C):
                below = src[c, b, sl(r0, 1), :]
                rightv = jnp.where(last, rolled[(c + 1) % C], rolled[c])
                qx = MX[k, c] * (below - ub[c])
                qy = MY[k, c] * (rightv - ub[c])
                if it > 0:
                    sc = SC[it - 1, c, sl(r0), :]
                    qx = qx + sc * QX[c, b, sl(r0), :]
                    qy = qy + sc * QY[c, b, sl(r0), :]
                QX[c, b, sl(r0), :] = qx
                QY[c, b, sl(r0), :] = qy
                if r0 == T2:
                    QX[c, b, 0:8, :] = qx
                elif it == 0 and r0 == O0:
                    N[c, b, 32:40, :] = ub[c]
                if r0 != T2:
                    out.append(acc[c] + (qx * qx + qy * qy))
            return tuple(out)

        init = () if r0 == T2 else (jnp.zeros((8, LANES), F32),) * C
        acc = lax.fori_loop(0, NB, body, init, unroll=UNROLL_B)
        if r0 != T2:
            for c in range(C):
                SB[it, k * C + c] = acc[c]

    def primal(it, r0):
        sc = [SC[it, c, sl(r0), :] for c in range(C)]
        keep = it == 0 and r0 != O0
        through = it == 0 and r0 == T2
        scu = None if through else [SC[it, c, sl(r0, -1), :] for c in range(C)]

        def body(b, carry):
            py = [sc[c] * QY[c, b, sl(r0), :] for c in range(C)]
            rolled = [pltpu.roll(v, 1, 1) for v in py]
            px = [sc[c] * QX[c, b, sl(r0), :] for c in range(C)]
            if keep:
                for c in range(C):
                    PX[c, b, sl(r0), :] = px[c]
            for c in range(C):
                if through:
                    pxu = PX[c, b, sl(r0, -1), :]
                else:
                    pxu = scu[c] * QX[c, b, sl(r0, -1), :]
                pyl = jnp.where(first, rolled[(c - 1) % C], rolled[c])
                div = (px[c] - pxu) + (py[c] - pyl)
                n = N[c, b, sl(r0), :]
                if it == 0:
                    old = n
                    new = n + div
                else:
                    old = U[c, b, sl(r0), :]
                    new = C0 * old + (KAPPA * n + div)
                ubar = 2.0 * new - old
                U[c, b, sl(r0), :] = new
                UB[c, b, sl(r0), :] = ubar
                if r0 == O0:
                    UB[c, b, 32:40, :] = ubar
            return carry

        lax.fori_loop(0, NB, body, 0, unroll=UNROLL_A)

    def final(it, r0, own):
        sc = [SC[it, c, sl(r0), :] for c in range(C)]
        scu = [SC[it, c, sl(r0, -1), :] for c in range(CT)]
        base = (core if own else 1 - core) * bands

        def body(i, carry):
            b = base + i
            py = [sc[c] * QY[c, b, sl(r0), :] for c in range(C)]
            rolled = [pltpu.roll(v, 1, 1) for v in py]
            for c in range(CT):
                px = sc[c] * QX[c, b, sl(r0), :]
                pxu = scu[c] * QX[c, b, sl(r0, -1), :]
                pyl = jnp.where(first, rolled[(c - 1) % C], rolled[c])
                div = (px - pxu) + (py[c] - pyl)
                new = C0 * U[c, b, sl(r0), :] + (KAPPA * N[c, b, sl(r0), :] + div)
                if own:
                    out_ref[i, r0 - 8 : r0, lanes_of(core, c)] = new
                else:
                    OUT[c, i, r0 - 8 : r0, :] = new
            return carry

        lax.fori_loop(0, bands, body, 0, unroll=UNROLL_A)

    pending = list(swaps) + strips + nexts + margins

    def step(it, n, h):
        src, dst = ((SB, RB1), (TB, RB2))[n]
        a, b = h * C, h * C + C
        return remote(src.at[it, a:b], dst.at[it, a:b], ar_s.at[it, n, h], ar_r.at[it, n, h], (zA, zB)[(n + h) % 2])

    steps = [[[step(it, n, h) for h in range(2)] for n in range(2)] for it in range(ITERS)]

    def edge(it, h, n):
        if h == 0:
            src, dst, to = TB.at[it, 0:C, 0:M, :], ELO.at[it, n, :, 0:M, :], (up, up_zB)[n]
        else:
            src, dst, to = TB.at[it, C : 2 * C, 8 - M : 8, :], EUP.at[it, n, :, 8 - M : 8, :], (down, down_zA)[n]
        return remote(src, dst, e_s.at[it, h, n], e_r.at[it, h, n], to)

    edges = [[[edge(it, h, n) for n in range(2)] for h in range(2)] for it in range(ITERS)]

    def forward(it, h):
        steps[it][0][h].wait_recv()
        for t in range(h * C, h * C + C):
            TB[it, t] = SB[it, t] + RB1[it, t]
        steps[it][1][h].start()
        if h == 1 or it < ITERS - 1:
            for cp in edges[it][h]:
                cp.start()
                pending.append(cp)

    def scale_of(w, s):
        return w / jnp.maximum(w, jnp.sqrt(1.0 + s * (1.0 / (KAPPA * KAPPA))))

    def scales(it, h):
        steps[it][1][h].wait_recv()
        r0 = (O0, O1)[h]
        for c in range(C):
            t = h * C + c
            SC[it, c, sl(r0), :] = scale_of(N[c, NB, sl(r0), :], TB[it, t] + RB2[it, t])

    def scales_above(it):
        for cp in edges[it][1]:
            cp.wait_recv()
        for c in range(C):
            SC[it, c, 0:8, :] = scale_of(N[c, NB, sl(T2), :], EUP[it, 0, c] + EUP[it, 1, c])

    def scales_margin(it):
        for cp in edges[it][0]:
            cp.wait_recv()
        for c in range(C):
            lo = scale_of(N[c, NB, sl(T2), :], ELO[it, 0, c] + ELO[it, 1, c])
            SC[it, c, sl(T2), :] = jnp.where(sub < M, lo, SC[it, c, 0:8, :])

    for side, src in ((core, 1 - core), (1 - core, 0), (1 - core, 1)):
        strip_arrival(side, src, 0).wait_recv()
    unpack((0, 1))
    dual(0, O0)
    steps[0][0][0].start()
    for side in range(2):
        for src in range(2):
            for part in (1, 2):
                strip_arrival(side, src, part).wait_recv()
    unpack((2,))
    for t in range(2):
        for c in range(CT):
            next_row_arrival(0, t, c).wait_recv()
    dual(0, O1)
    steps[0][0][1].start()
    margins[1].start()
    for it in range(ITERS):
        pending += steps[it][0] + steps[it][1]
        order = (0, 1) if it == 0 else (1, 0)
        for h in order:
            forward(it, h)
        if it == 0:
            for cp in margins[2:5]:
                cp.start()
        if it == 1:
            for cp in margins[2:6]:
                cp.wait_recv()
            mid = (sub >= 2) & (sub < 6)

            def merge(b, carry):
                for c in range(CT):
                    N[c, b, sl(T2), :] = jnp.where(mid, N2[c, b], N[c, b, sl(T2), :])
                return carry

            lax.fori_loop(0, NB, merge, 0, unroll=8)
            dual(0, T2)
            primal(0, T2)
            dual(1, T2)
        for h in order:
            scales(it, h)
        if it == ITERS - 1:
            final(it, O1, False)
            outs = [
                remote(OUT.at[c, :, 8 * h : 8 * h + 8, :], out_ref.at[:, 8 * h : 8 * h + 8, lanes_of(core, c)], o_s.at[h, c], o_r.at[h, c], partner)
                for h in (1, 0) for c in range(CT)
            ]
            for cp in outs[:CT]:
                cp.start()
            scales_above(it)
            final(it, O0, False)
            for cp in outs[CT:]:
                cp.start()
            final(it, O1, True)
            final(it, O0, True)
            continue
        primal(it, O1)
        if it == 0:
            for t in range(2):
                for c in range(CT):
                    next_row_arrival(1, t, c).wait_recv()
            for cp in margins[0:2] + margins[6:8]:
                cp.wait_recv()
            dual(0, T2)
        scales_above(it)
        primal(it, O0)
        scales_margin(it)
        primal(it, T2)
        dual(it + 1, O1)
        steps[it + 1][0][1].start()
        dual(it + 1, O0)
        steps[it + 1][0][0].start()
        if it == 0:
            margins[5].start()
        dual(it + 1, T2)

    for cp in pending:
        cp.wait_send()
    for cp in outs:
        cp.wait()


def solution(mesh):
    dims = tuple(mesh.shape[a] for a in ("row", "col", "band"))

    def local(noisy, weight_map):
        bands, rows, cols = noisy.shape
        NB = 2 * bands
        CT = cols // 2 // LANES
        C = CT + 1
        vm = lambda *s: pltpu.VMEM(s, F32)
        big = lambda: vm(C, NB + 1, SROWS, LANES)
        dma = lambda *s: pltpu.SemaphoreType.DMA(s)
        half_sums = lambda: vm(ITERS, 2 * C, 8, LANES)
        return pl.pallas_call(
            functools.partial(kernel, dims),
            out_shape=jax.ShapeDtypeStruct(noisy.shape, F32),
            in_specs=[pl.BlockSpec(memory_space=pl.ANY)] * 2,
            out_specs=pl.BlockSpec(memory_space=pltpu.VMEM),
            scratch_shapes=[
                big(), vm(CT, NB, 8, LANES), big(), big(), big(), big(), big(),
                vm(ITERS, C, SROWS, LANES), vm(ITERS, 2, C, 8, LANES), vm(ITERS, 2, C, 8, LANES),
                vm(3, C, 8, LANES), vm(3, C, 8, LANES), vm(CT, bands, rows, LANES),
                vm(2, bands, rows, LANES), vm(4, rows, LANES), vm(2, 2, rows + 2 * M, LANES),
                half_sums(), half_sums(), half_sums(), half_sums(),
                dma(CT), dma(CT), dma(2), dma(CT), dma(CT), dma(2, 2, CT), dma(2, 2, CT), dma(8), dma(8), dma(4, 3), dma(2, 2, 3),
                dma(ITERS, 2, 2), dma(ITERS, 2, 2), dma(ITERS, 2, 2), dma(ITERS, 2, 2), dma(2, CT), dma(2, CT),
            ],
            compiler_params=pltpu.CompilerParams(
                collective_id=0, has_side_effects=True, vmem_limit_bytes=52 * 1024 * 1024
            ),
        )(noisy, weight_map)

    return jax.shard_map(
        local, mesh=mesh, in_specs=(P("band", "row", "col"), P("row", "col")),
        out_specs=P("band", "row", "col"), check_vma=False,
    )
```
